32 devices in a mesh: dp: 4 (over y, z), cp: 8 (over x, core).
Axes of the slice: x: 4, y: 2, z: 2, core: 2. Of those that a mesh axis runs over, the one named last changes fastest.
The devices are a block of a 4x4x8 slice.
Arguments:
- latent: bfloat16 [64, 6, 96, 512], P(('dp', 'cp')), parts along dimension 0
- conv_kernels: bfloat16 [4, 3, 3, 3, 512, 512], replicated
- conv_biases: float32 [4, 512], replicated
- gn_gammas: float32 [4, 512], replicated
- gn_betas: float32 [4, 512], replicated
Outputs:
- output: bfloat16 [64, 6, 96, 512], P(('dp', 'cp')), parts along dimension 0
There are 4 independent parts. The reference program is written for one: setup_inputs(seed, part) draws one part's arguments, and reference() takes and returns one part's arrays. A program takes and returns all parts, laid end to end along the dimension named above; an argument that names none is the same for every part.
All inputs are finite; a program needn't handle non-finite values.
Results may differ from the reference program's by a relative error of at most 0.0124199.
Values are sent between devices in bfloat16 or wider.
A program may use at most 768 MiB of HBM per device.

```python
import jax
import jax.numpy as jnp
from jax import lax

FRAMES = 16
LAT_HEIGHT = 6
LAT_WIDTH = 96
CHANNELS = 512
GROUPS = 32
NORM_EPS = 1e-6


def setup_inputs(seed: int = 0, part: int = 0) -> dict:
    part_key = jax.random.fold_in(jax.random.key(seed), part)
    key_noise, key_slope, key_jitter, key_gain = jax.random.split(part_key, 4)
    key_kernel, key_bias, key_gamma, key_beta = jax.random.split(jax.random.key(seed + 1), 4)
    time_trend = jnp.linspace(-1.0, 1.0, FRAMES)
    chan_slope = jax.random.normal(key_slope, (CHANNELS,))
    frame_mean = time_trend[:, None] * chan_slope[None, :] + 0.3 * jax.random.normal(key_jitter, (FRAMES, CHANNELS))
    frame_gain = jnp.exp(0.5 * time_trend + 0.2 * jax.random.normal(key_gain, (FRAMES,)))
    base_noise = jax.random.normal(key_noise, (FRAMES, LAT_HEIGHT, LAT_WIDTH, CHANNELS))
    latent = base_noise * frame_gain[:, None, None, None] + frame_mean[:, None, None, :]
    conv_kernels = jax.random.normal(key_kernel, (4, 3, 3, 3, CHANNELS, CHANNELS)) * (27 * CHANNELS) ** -0.5
    conv_biases = 0.3 * jax.random.normal(key_bias, (4, CHANNELS))
    gn_gammas = 1.0 + 0.3 * jax.random.normal(key_gamma, (4, CHANNELS))
    gn_betas = 0.3 * jax.random.normal(key_beta, (4, CHANNELS))
    return {"latent": latent.astype(jnp.bfloat16), "conv_kernels": conv_kernels.astype(jnp.bfloat16), "conv_biases": conv_biases.astype(jnp.float32), "gn_gammas": gn_gammas.astype(jnp.float32), "gn_betas": gn_betas.astype(jnp.float32)}


def norm_act(hidden, gn_gamma, gn_beta):
    widened = hidden.astype(jnp.float32)
    grouped = widened.reshape(hidden.shape[:-1] + (GROUPS, CHANNELS // GROUPS))
    elem_count = grouped.size // GROUPS
    sum_one = jnp.sum(grouped, axis=(0, 1, 2, 4))
    sum_sq = jnp.sum(grouped * grouped, axis=(0, 1, 2, 4))
    grp_mean = sum_one / elem_count
    grp_var = sum_sq / elem_count - grp_mean * grp_mean
    normed = (grouped - grp_mean[:, None]) * lax.rsqrt(grp_var + NORM_EPS)[:, None]
    normed = (normed.reshape(hidden.shape) * gn_gamma + gn_beta).astype(jnp.bfloat16)
    return jax.nn.silu(normed.astype(jnp.float32)).astype(jnp.bfloat16)


def causal_conv(act_in, kernel, conv_bias):
    padded = jnp.concatenate([act_in[:1], act_in[:1], act_in], axis=0).astype(jnp.float32)
    result = lax.conv_general_dilated(padded[None], kernel.astype(jnp.float32), (1, 1, 1), ((0, 0), (1, 1), (1, 1)), dimension_numbers=("NDHWC", "DHWIO", "NDHWC"))[0]
    return (result + conv_bias).astype(jnp.bfloat16)


def reference(latent, conv_kernels, conv_biases, gn_gammas, gn_betas):
    def block_step(hidden, block_params):
        kernel_pair, bias_pair, gamma_pair, beta_pair = block_params
        inner = causal_conv(norm_act(hidden, gamma_pair[0], beta_pair[0]), kernel_pair[0], bias_pair[0])
        inner = causal_conv(norm_act(inner, gamma_pair[1], beta_pair[1]), kernel_pair[1], bias_pair[1])
        return (hidden.astype(jnp.float32) + inner.astype(jnp.float32)).astype(jnp.bfloat16), None

    block_params = (conv_kernels.reshape((2, 2) + conv_kernels.shape[1:]), conv_biases.reshape(2, 2, CHANNELS), gn_gammas.reshape(2, 2, CHANNELS), gn_betas.reshape(2, 2, CHANNELS))
    decoded, _ = lax.scan(block_step, latent, block_params)
    return decoded
```

```python
import functools

import jax
import jax.numpy as jnp
from jax import lax
from jax.experimental import pallas as pl
from jax.experimental.pallas import tpu as pltpu
from jax.sharding import PartitionSpec as P

GROUPS = 32
NORM_EPS = 1e-6
N_LAYERS = 4
HALF = 256
SKEW = 1
MESH = pl.DeviceIdType.MESH


def interleave(long, short):
    if not short:
        return list(long)
    out, taken = [], 0
    for idx, job in enumerate(long):
        due = (idx * len(short)) // max(len(long), 1) + 1
        while taken < min(due, len(short)):
            out.append(short[taken])
            taken += 1
        out.append(job)
    return out + list(short[taken:])


def make_kernel(n_ranks, n_frames, n_rows, n_cols, n_chans):
    width = n_chans // GROUPS
    elem_count = float(n_ranks * n_frames * n_rows * n_cols * width)
    halves = n_chans // HALF

    def kernel(latent, weights, biases, gammas, betas, out, wbuf, act_l, act_c, act_r, raw, stat, sums, coef,
               w_sem, lat_sem, out_sem, halo_send, halo_recv, st_send, st_recv):
        acts = {-1: act_l, 0: act_c, 1: act_r}
        me = lax.axis_index("cp")
        is_first = me == 0
        has_next = me < n_ranks - 1

        def weight_copy(layer, slot, k):
            return pltpu.make_async_copy(weights.at[layer, pl.ds(9 * k, 9)], wbuf.at[slot, pl.ds(9 * k, 9)], w_sem.at[slot, k])

        def latent_copy(row):
            return pltpu.make_async_copy(latent.at[:, row], raw.at[0, row, pl.ds(2, n_frames)], lat_sem.at[row])

        def out_copy(row):
            return pltpu.make_async_copy(raw.at[0, row, pl.ds(2, n_frames)], out.at[:, row], out_sem.at[row])

        def halo_copy(layer, slot, row):
            return pltpu.make_async_remote_copy(
                src_ref=raw.at[slot, row, pl.ds(2, n_frames)], dst_ref=raw.at[slot, row, pl.ds(0, n_frames)],
                send_sem=halo_send.at[layer, row], recv_sem=halo_recv.at[layer, row],
                device_id={"cp": me + 1}, device_id_type=MESH)

        def stat_copy(layer, hop):
            return pltpu.make_async_remote_copy(
                src_ref=stat.at[layer, me], dst_ref=stat.at[layer, me],
                send_sem=st_send.at[layer, hop - 1], recv_sem=st_recv.at[layer, hop - 1],
                device_id={"cp": lax.rem(me + hop, n_ranks)}, device_id_type=MESH)

        def send_stats(layer):
            stat[layer, me, 0:1, :] = jnp.sum(sums[0], axis=0, keepdims=True)
            stat[layer, me, 1:2, :] = jnp.sum(sums[1], axis=0, keepdims=True)
            for hop in range(1, n_ranks):
                stat_copy(layer, hop).start()

        def add_sums(val, cols):
            slabs = val.reshape(n_cols // 8, 8, val.shape[-1])
            sums[0, :, cols] += jnp.sum(slabs, axis=0)
            sums[1, :, cols] += jnp.sum(slabs * slabs, axis=0)

        def body():
            for row in range(n_rows):
                latent_copy(row).start()
            for k in (2, 1, 0):
                weight_copy(0, 0, k).start()
            barrier = pltpu.get_barrier_semaphore()
            for hop in range(1, n_ranks):
                pl.semaphore_signal(barrier, inc=1, device_id={"cp": lax.rem(me + hop, n_ranks)}, device_id_type=MESH)
            sums[...] = jnp.zeros_like(sums)
            for row in range(n_rows):
                latent_copy(row).wait()
                for frame in range(n_frames):
                    for half in range(halves):
                        cols = pl.ds(half * HALF, HALF)
                        add_sums(raw[0, row, 2 + frame, :, cols].astype(jnp.float32), cols)
            pl.semaphore_wait(barrier, n_ranks - 1)
            send_stats(0)

            @pl.when(has_next)
            def _():
                for row in range(n_rows):
                    halo_copy(0, 0, row).start()

            def layer_step(layer, carry):
                slot = lax.rem(layer, 2)
                other = 1 - slot
                adds_input = slot == 1
                last = layer == N_LAYERS - 1

                @pl.when(jnp.logical_not(last))
                def _():
                    for k in (2, 1, 0):
                        weight_copy(layer + 1, other, k).start()

                sums[...] = jnp.zeros_like(sums)
                for hop in range(1, n_ranks):
                    stat_copy(layer, hop).wait_recv()
                total = stat[layer, 0]
                for rank in range(1, n_ranks):
                    total = total + stat[layer, rank]
                lane = lax.broadcasted_iota(jnp.int32, total.shape, 1)
                step = 1
                while step < width:
                    lower = pltpu.roll(total, step, 1)
                    upper = pltpu.roll(total, n_chans - step, 1)
                    total = total + jnp.where(lax.rem(lax.div(lane, step), 2) == 0, upper, lower)
                    step *= 2
                mean = total[0:1] * (1.0 / elem_count)
                var = total[1:2] * (1.0 / elem_count) - mean * mean
                scale = lax.rsqrt(var + NORM_EPS) * gammas[pl.ds(layer, 1), :]
                coef[0:1, :] = scale
                coef[1:2, :] = betas[pl.ds(layer, 1), :] - mean * scale

                def act_piece(row, frame, half):
                    cols = pl.ds(half * HALF, HALF)
                    src = jnp.where(is_first, 2, frame) if frame < 2 else frame
                    val = raw[slot, row, src, :, cols].astype(jnp.float32)
                    normed = (val * coef[0:1, cols] + coef[1:2, cols]).astype(jnp.bfloat16).astype(jnp.float32)
                    arg = 0.5 * normed
                    res = arg * jnp.tanh(arg) + arg
                    act_c[row, frame, :, cols] = res.astype(jnp.bfloat16)
                    edge = lax.broadcasted_iota(jnp.int32, (16, HALF), 0)
                    moved = pltpu.roll(res, 1, 0)
                    act_l[row, frame, 0:16, cols] = jnp.where(edge == 0, 0.0, moved[:16]).astype(jnp.bfloat16)
                    act_l[row, frame, 16:n_cols, cols] = moved[16:].astype(jnp.bfloat16)
                    moved = pltpu.roll(res, n_cols - 1, 0)
                    act_r[row, frame, 0:n_cols - 16, cols] = moved[:n_cols - 16].astype(jnp.bfloat16)
                    act_r[row, frame, n_cols - 16:n_cols, cols] = jnp.where(edge == 15, 0.0, moved[n_cols - 16:]).astype(jnp.bfloat16)

                def act_jobs(row, local):
                    frames = (2, 3) if local else (0, 1)
                    return [functools.partial(act_piece, row, frame, half) for frame in frames for half in range(halves)]

                def out_piece(row, frame, mxu):
                    cols = pl.ds(mxu * HALF, HALF)
                    got = sums_of[row][frame * n_cols:(frame + 1) * n_cols, mxu * HALF:(mxu + 1) * HALF] + biases[pl.ds(layer, 1), cols]
                    inner = got.astype(jnp.bfloat16).astype(jnp.float32)
                    held = raw[other, row, 2 + frame, :, cols].astype(jnp.float32)
                    new = jnp.where(adds_input, held + inner, inner).astype(jnp.bfloat16)
                    raw[other, row, 2 + frame, :, cols] = new
                    add_sums(new.astype(jnp.float32), cols)

                def out_jobs(row):
                    return [functools.partial(out_piece, row, frame, mxu) for frame in range(n_frames) for mxu in range(halves)]

                def finish_row(row):
                    @pl.when(jnp.logical_and(jnp.logical_not(last), has_next))
                    def _():
                        halo_copy(layer + 1, other, row).start()

                    @pl.when(last)
                    def _():
                        out_copy(row).start()

                def taps(row, ks):
                    return [(row, k, di, dj) for k in ks for dj in (-1, 0, 1) for di in (-1, 0, 1) if 0 <= row + di < n_rows]

                segments = []
                for row in range(n_rows + SKEW):
                    if row < n_rows:
                        segments.append(("new", row))
                    if row >= SKEW:
                        segments.append(("old", row - SKEW))
                seq = [taps(row, (2,) if kind == "new" else (1, 0)) for kind, row in segments]
                flat = [tile for tiles in seq for tile in tiles]

                sums_of = {}

                def tile_job(idx):
                    row, k, di, dj = flat[idx]
                    lhs = acts[dj][row + di, pl.ds(k, n_frames)].reshape(n_frames * n_cols, n_chans)
                    part = jnp.dot(lhs, wbuf[slot, 9 * k + 3 * (di + 1) + dj + 1], preferred_element_type=jnp.float32)
                    sums_of[row] = part if row not in sums_of else sums_of[row] + part

                def wait_halo(row):
                    @pl.when(jnp.logical_not(is_first))
                    def _():
                        halo_copy(layer, slot, row).wait_recv()

                weight_copy(layer, slot, 2).wait()
                for row in (0, 1):
                    for job in act_jobs(row, True):
                        job()

                done, pending, idx = 0, None, 0
                for kind, row in segments:
                    side = []
                    if kind == "new" and row + 2 < n_rows:
                        side += act_jobs(row + 2, True)
                    if kind == "new" and row in (SKEW - 1, SKEW):
                        wait_halo(row - SKEW + 1)
                        side += act_jobs(row - SKEW + 1, False)
                    if kind == "old" and row == 0:
                        weight_copy(layer, slot, 1).wait()
                        weight_copy(layer, slot, 0).wait()
                    if kind == "old" and row + 2 < n_rows:
                        wait_halo(row + 2)
                        side += act_jobs(row + 2, False)
                    if pending is not None:
                        side = out_jobs(pending) + side
                    count = len(seq[segments.index((kind, row))])
                    for job in interleave([functools.partial(tile_job, idx + j) for j in range(count)], side):
                        job()
                    idx += count
                    if pending is not None:
                        finish_row(pending)
                        pending = None
                    if kind == "old":
                        pending = row
                for job in out_jobs(pending):
                    job()

                @pl.when(jnp.logical_not(last))
                def _():
                    send_stats(layer + 1)

                finish_row(pending)

                @pl.when(has_next)
                def _():
                    for row in range(n_rows):
                        halo_copy(layer, slot, row).wait_send()

                for hop in range(1, n_ranks):
                    stat_copy(layer, hop).wait_send()
                return carry

            lax.fori_loop(0, N_LAYERS, layer_step, 0)
            for row in range(n_rows):
                out_copy(row).wait()

        body()

    return kernel


def solution(mesh):
    n_ranks = mesh.shape["cp"]
    frame_spec = P(("dp", "cp"))

    def local_fn(latent, conv_kernels, conv_biases, gn_gammas, gn_betas):
        n_frames, n_rows, n_cols, n_chans = latent.shape
        weights = conv_kernels.reshape(N_LAYERS, 27, n_chans, n_chans)
        act_shape = pltpu.VMEM((n_rows, 4, n_cols, n_chans), jnp.bfloat16)
        return pl.pallas_call(
            make_kernel(n_ranks, n_frames, n_rows, n_cols, n_chans),
            out_shape=jax.ShapeDtypeStruct(latent.shape, latent.dtype),
            in_specs=[pl.BlockSpec(memory_space=pl.ANY)] * 2 + [pl.BlockSpec(memory_space=pltpu.VMEM)] * 3,
            out_specs=pl.BlockSpec(memory_space=pl.ANY),
            scratch_shapes=[
                pltpu.VMEM((2, 27, n_chans, n_chans), jnp.bfloat16),
                act_shape, act_shape, act_shape,
                pltpu.VMEM((2, n_rows, 4, n_cols, n_chans), jnp.bfloat16),
                pltpu.VMEM((N_LAYERS, n_ranks, 2, n_chans), jnp.float32),
                pltpu.VMEM((2, 8, n_chans), jnp.float32),
                pltpu.VMEM((2, n_chans), jnp.float32),
                pltpu.SemaphoreType.DMA((2, 3)),
                pltpu.SemaphoreType.DMA((n_rows,)),
                pltpu.SemaphoreType.DMA((n_rows,)),
                pltpu.SemaphoreType.DMA((N_LAYERS, n_rows)),
                pltpu.SemaphoreType.DMA((N_LAYERS, n_rows)),
                pltpu.SemaphoreType.DMA((N_LAYERS, n_ranks - 1)),
                pltpu.SemaphoreType.DMA((N_LAYERS, n_ranks - 1)),
            ],
            compiler_params=pltpu.CompilerParams(collective_id=0, has_side_effects=True, vmem_limit_bytes=60 * 1024 * 1024),
            name="decode",
        )(latent, weights, conv_biases, gn_gammas, gn_betas)

    return jax.shard_map(local_fn, mesh=mesh, in_specs=(frame_spec, P(), P(), P(), P()), out_specs=frame_spec, check_vma=False)
```

```python
import functools

import jax
import jax.numpy as jnp
from jax import lax
from jax.experimental import pallas as pl
from jax.experimental.pallas import tpu as pltpu
from jax.sharding import PartitionSpec as P

GROUPS = 32
NORM_EPS = 1e-6
N_LAYERS = 4
HALF = 256
MESH = pl.DeviceIdType.MESH


def interleave(long, short):
    if not short:
        return list(long)
    out, taken = [], 0
    for idx, job in enumerate(long):
        due = (idx * len(short)) // max(len(long), 1) + 1
        while taken < min(due, len(short)):
            out.append(short[taken])
            taken += 1
        out.append(job)
    return out + list(short[taken:])


def make_kernel(n_ranks, n_frames, n_rows, n_cols, n_chans):
    width = n_chans // GROUPS
    elem_count = float(n_ranks * n_frames * n_rows * n_cols * width)
    halves = n_chans // HALF
    pairs = [((row,), (row + 1,)) for row in range(1, n_rows - 1, 2)] + [((0,), (n_rows - 1,))]
    block = n_frames * n_cols

    def kernel(latent, weights, biases, gammas, betas, out, wbuf, act_0l, act_0c, act_0r, act_1l, act_1c, act_1r, raw, part, stat,
               sums, coef, w_sem, lat_sem, halo_send, halo_recv, st_send, st_recv):
        acts = ({-1: act_0l, 0: act_0c, 1: act_0r}, {-1: act_1l, 0: act_1c, 1: act_1r})
        me = lax.axis_index("cp")
        is_first = me == 0
        nought = lax.rem(me * (me + 1), 2)

        def weight_copy(layer, slot, k):
            return pltpu.make_async_copy(weights.at[layer, pl.ds(9 * k, 9)], wbuf.at[slot, pl.ds(9 * k, 9)], w_sem.at[slot, k])

        def latent_copy(half, row):
            return pltpu.make_async_copy(latent.at[:, row, :, pl.ds(half * HALF, HALF)],
                                         raw.at[0, half, row, pl.ds(2, n_frames)], lat_sem.at[half, row])

        def out_copy(half, row):
            return pltpu.make_async_copy(raw.at[0, half, row, pl.ds(2, n_frames)],
                                         out.at[:, row, :, pl.ds(half * HALF, HALF)], lat_sem.at[half, row])

        def halo_copy(layer, slot, half, row):
            return pltpu.make_async_remote_copy(
                src_ref=raw.at[slot, half, row, pl.ds(2, n_frames)], dst_ref=raw.at[slot, half, row, pl.ds(0, n_frames)],
                send_sem=halo_send.at[slot, half, row], recv_sem=halo_recv.at[slot, half, row],
                device_id={"cp": lax.rem(me + 1, n_ranks)}, device_id_type=MESH)

        def stat_copy(layer, half, hop):
            turn = layer % 2 if isinstance(layer, int) else lax.rem(layer, 2)
            return pltpu.make_async_remote_copy(
                src_ref=stat.at[layer, half, me], dst_ref=stat.at[layer, half, me],
                send_sem=st_send.at[turn, half, hop - 1], recv_sem=st_recv.at[turn, half, hop - 1],
                device_id={"cp": lax.rem(me + hop, n_ranks)}, device_id_type=MESH)

        def send_stats(layer, half):
            stat[layer, half, me, 0:1, :] = jnp.sum(sums[half, 0], axis=0, keepdims=True)
            stat[layer, half, me, 1:2, :] = jnp.sum(sums[half, 1], axis=0, keepdims=True)
            for hop in range(1, n_ranks):
                stat_copy(layer, half, hop).start()

        def clear_sums(half):
            sums[half] = jnp.zeros(sums.shape[1:], sums.dtype)

        def add_sums(val, half):
            slabs = val.reshape(n_cols // 8, 8, val.shape[-1])
            sums[half, 0] += jnp.sum(slabs, axis=0)
            sums[half, 1] += jnp.sum(slabs * slabs, axis=0)

        def take_stats(layer, param, half):
            for hop in range(1, n_ranks):
                stat_copy(layer, half, hop).wait_recv()
            total = stat[layer, half, 0]
            for rank in range(1, n_ranks):
                total = total + stat[layer, half, rank]
            lane = lax.broadcasted_iota(jnp.int32, total.shape, 1)
            step = 1
            while step < width:
                lower = pltpu.roll(total, step, 1)
                upper = pltpu.roll(total, HALF - step, 1)
                total = total + jnp.where(lax.rem(lax.div(lane, step), 2) == 0, upper, lower)
                step *= 2
            cols = pl.ds(half * HALF, HALF)
            mean = total[0:1] * (1.0 / elem_count)
            var = total[1:2] * (1.0 / elem_count) - mean * mean
            scale = lax.rsqrt(var + NORM_EPS) * gammas[pl.ds(param, 1), cols]
            coef[half, 0:1, :] = scale
            coef[half, 1:2, :] = betas[pl.ds(param, 1), cols] - mean * scale

        def act_piece(slot, half, row, frame):
            left, centre, right = acts[half][-1], acts[half][0], acts[half][1]
            src = jnp.where(is_first, 2, frame) if frame < 2 else frame
            val = raw[slot, half, row, src].astype(jnp.float32)
            normed = (val * coef[half, 0:1] + coef[half, 1:2]).astype(jnp.bfloat16).astype(jnp.float32)
            arg = 0.5 * normed
            res = arg * jnp.tanh(arg) + arg
            centre[row, frame] = res.astype(jnp.bfloat16)
            edge = lax.broadcasted_iota(jnp.int32, (16, HALF), 0)
            moved = pltpu.roll(res, 1, 0)
            left[row, frame, 0:16] = jnp.where(edge == 0, 0.0, moved[:16]).astype(jnp.bfloat16)
            left[row, frame, 16:n_cols] = moved[16:].astype(jnp.bfloat16)
            moved = pltpu.roll(res, n_cols - 1, 0)
            right[row, frame, 0:n_cols - 16] = moved[:n_cols - 16].astype(jnp.bfloat16)
            right[row, frame, n_cols - 16:n_cols] = jnp.where(edge == 15, 0.0, moved[n_cols - 16:]).astype(jnp.bfloat16)

        def act_jobs(slot, half, row, local):
            return [functools.partial(act_piece, slot, half, row, frame) for frame in ((2, 3) if local else (0, 1))]

        for half in range(halves):
            for row in range(n_rows):
                latent_copy(half, row).start()
        for k in (2, 1, 0):
            weight_copy(0, 0, k).start()
        barrier = pltpu.get_barrier_semaphore()
        for hop in range(1, n_ranks):
            pl.semaphore_signal(barrier, inc=1, device_id={"cp": lax.rem(me + hop, n_ranks)}, device_id_type=MESH)
        for half in range(halves):
            clear_sums(half)
            for row in range(n_rows):
                latent_copy(half, row).wait()
                for frame in range(n_frames):
                    add_sums(raw[0, half, row, 2 + frame].astype(jnp.float32), half)
        pl.semaphore_wait(barrier, n_ranks - 1)
        for half in range(halves):
            send_stats(0, half)
        for half in range(halves):
            for row in range(n_rows):
                halo_copy(0, 0, half, row).start()
        take_stats(0, 0, 0)
        for row in range(2):
            for job in act_jobs(0, 0, row, True):
                job()

        def layer_step(layer, carry):
            slot = lax.rem(layer, 2)
            other = 1 - slot
            adds_input = slot == 1
            last = layer == N_LAYERS - 1

            @pl.when(jnp.logical_not(last))
            def _():
                for k in (2, 1, 0):
                    weight_copy(layer + 1, other, k).start()

            vals = {}

            def accumulate(key, lhs, tap, in_half, cols, where=None):
                term = jnp.dot(lhs, wbuf[slot if where is None else where, tap, pl.ds(in_half * HALF, HALF), cols], preferred_element_type=jnp.float32)
                vals[key] = term if key not in vals else vals[key] + term

            def taps(k):
                return [(di, dj, 9 * k + 3 * (di + 1) + dj + 1) for dj in (-1, 0, 1) for di in (0, 1, -1)]

            def row_tile(key, row, k, di, dj, tap, in_half):
                lhs = acts[in_half][dj][row + di, pl.ds(k, n_frames)].reshape(block, HALF)
                accumulate(key, lhs, tap, in_half, pl.ds(0, n_chans))

            def row_chain(key, row, k, in_half):
                return [functools.partial(row_tile, key, row, k, di, dj, tap, in_half)
                        for di, dj, tap in taps(k) if 0 <= row + di < n_rows]

            def set_tile(tag, rows, di, dj, tap, in_half, out_half):
                inside = [row for row in rows if 0 <= row + di < n_rows]
                count = len(inside)
                lhs = acts[in_half][dj][pl.ds(inside[0] + di, count), pl.ds(tap // 9, n_frames)].reshape(count * block, HALF)
                accumulate((tag, rows), lhs, tap, in_half, pl.ds(out_half * HALF, HALF))

            def pair_chain(tag, pair, k, in_half, out_half):
                streams = [[functools.partial(set_tile, tag, rows, di, dj, tap, in_half, out_half) for di, dj, tap in taps(k)
                            if any(0 <= row + di < n_rows for row in rows)] for rows in pair]
                return [job for jobs in zip(*streams) for job in jobs]

            def keep_piece(key, row, frame, first, cols):
                span = slice(frame * n_cols, (frame + 1) * n_cols)
                got = vals[key][span]
                part[row, span, cols] = got if first else part[row, span, cols] + got

            def keep_jobs(key, row, first, half=None):
                cols = pl.ds(0, n_chans) if half is None else pl.ds(half * HALF, HALF)
                return [functools.partial(keep_piece, key, row, frame, first, cols) for frame in range(n_frames)]

            def out_piece(tag, rows, row, half, frame):
                span = slice(frame * n_cols, (frame + 1) * n_cols)
                base = (row - rows[0]) * block + frame * n_cols
                cols = pl.ds(half * HALF, HALF)
                got = jnp.where(nought == 0, vals[tag, rows][base:base + n_cols], 0.0) + part[row, span, cols] + biases[pl.ds(layer, 1), cols]
                inner = got.astype(jnp.bfloat16).astype(jnp.float32)
                held = raw[other, half, row, 2 + frame].astype(jnp.float32)
                new = jnp.where(adds_input, held + inner, inner).astype(jnp.bfloat16)
                raw[other, half, row, 2 + frame] = new
                add_sums(new.astype(jnp.float32), half)

            def out_jobs(tag, pair, half):
                return [functools.partial(out_piece, tag, rows, row, half, frame)
                        for rows in pair for row in rows for frame in range(n_frames)]

            def send_jobs(half, rows):
                return [lambda row=row: halo_copy(layer + 1, other, half, row).start() for row in rows]

            def halo_jobs(half, row):
                return [lambda: halo_copy(layer, slot, half, row).wait_recv()] + act_jobs(slot, half, row, False)

            def run(tiles, side=()):
                for job in interleave(tiles, list(side)):
                    job()

            later = []
            spread = [[(0, 1)], [(2,)], [(3,)], [(4,)], [(5,)]]
            for k in (2, 1, 0):
                weight_copy(layer, slot, k).wait()
                for row in range(n_rows):
                    key = ("row", k, row)
                    side = later
                    if k == 2 and row + 2 < n_rows:
                        side = side + act_jobs(slot, 0, row + 2, True)
                    if k == 2 and row >= n_rows - 2:
                        side = side + halo_jobs(0, row - n_rows + 2)
                    if k == 1 and row + 2 < n_rows:
                        side = side + halo_jobs(0, row + 2)
                    if k == 0 and row == 1:
                        side = side + [functools.partial(take_stats, layer, layer, 1)]
                    if k == 0 and row >= 1:
                        side = side + [job for rows in spread[row - 1] for got in rows for job in act_jobs(slot, 1, got, True)]
                    run(row_chain(key, row, k, 0), side)
                    later = keep_jobs(key, row, k == 2)

            clear_sums(0)
            for idx, pair in enumerate(pairs):
                tag = ("first", idx)
                ready = [(0, 1, 2, 3), (4, 5), ()][idx]
                run(pair_chain(tag, pair, 2, 1, 0), [job for row in ready for job in halo_jobs(1, row)])
                run(pair_chain(tag, pair, 1, 1, 0) + pair_chain(tag, pair, 0, 1, 0), later)
                later = out_jobs(tag, pair, 0) + (send_jobs(0, (1, 2)) if idx == 0 else [])

            later = later + [functools.partial(send_stats, layer + 1, 0), functools.partial(clear_sums, 1)]
            later = later + send_jobs(0, (0, 3, 4, 5))
            for idx, pair in enumerate(pairs):
                tag = ("second", idx)
                early = later if idx == 0 else []
                run(pair_chain(tag, pair, 2, 1, 1), early)
                run(pair_chain(tag, pair, 1, 1, 1) + pair_chain(tag, pair, 0, 1, 1), [] if idx == 0 else later)
                later = out_jobs(tag, pair, 1)
            for job in later:
                job()

            @pl.when(jnp.logical_not(last))
            def _():
                send_stats(layer + 1, 1)

            @pl.when(jnp.logical_not(last))
            def _():
                for row in range(n_rows):
                    halo_copy(layer + 1, other, 1, row).start()

            @pl.when(last)
            def _():
                for half in range(halves):
                    for row in range(n_rows):
                        out_copy(half, row).start()

            take_stats(layer + 1, jnp.minimum(layer + 1, N_LAYERS - 1), 0)
            for row in range(2):
                for job in act_jobs(other, 0, row, True):
                    job()

            for half in range(halves):
                for row in range(n_rows):
                    halo_copy(layer, slot, half, row).wait_send()
                for hop in range(1, n_ranks):
                    stat_copy(layer, half, hop).wait_send()
            return carry

        lax.fori_loop(0, N_LAYERS, layer_step, 0)
        for hop in range(1, n_ranks):
            stat_copy(N_LAYERS, 0, hop).wait_send()
        for row in range(n_rows):
            halo_copy(N_LAYERS, 0, 0, row).wait_send()
            halo_copy(N_LAYERS, 0, 0, row).wait_recv()
        for half in range(halves):
            for row in range(n_rows):
                out_copy(half, row).wait()

    return kernel


def solution(mesh):
    n_ranks = mesh.shape["cp"]
    frame_spec = P(("dp", "cp"))

    def local_fn(latent, conv_kernels, conv_biases, gn_gammas, gn_betas):
        n_frames, n_rows, n_cols, n_chans = latent.shape
        weights = conv_kernels.reshape(N_LAYERS, 27, n_chans, n_chans)
        halves = n_chans // HALF
        act_shape = pltpu.VMEM((n_rows, 4, n_cols, HALF), jnp.bfloat16)
        return pl.pallas_call(
            make_kernel(n_ranks, n_frames, n_rows, n_cols, n_chans),
            out_shape=jax.ShapeDtypeStruct(latent.shape, latent.dtype),
            in_specs=[pl.BlockSpec(memory_space=pl.ANY)] * 2 + [pl.BlockSpec(memory_space=pltpu.VMEM)] * 3,
            out_specs=pl.BlockSpec(memory_space=pl.ANY),
            scratch_shapes=[
                pltpu.VMEM((2, 27, n_chans, n_chans), jnp.bfloat16),
                act_shape, act_shape, act_shape, act_shape, act_shape, act_shape,
                pltpu.VMEM((2, halves, n_rows, 4, n_cols, HALF), jnp.bfloat16),
                pltpu.VMEM((n_rows, n_frames * n_cols, n_chans), jnp.float32),
                pltpu.VMEM((N_LAYERS + 1, halves, n_ranks, 2, HALF), jnp.float32),
                pltpu.VMEM((halves, 2, 8, HALF), jnp.float32),
                pltpu.VMEM((halves, 2, HALF), jnp.float32),
                pltpu.SemaphoreType.DMA((2, 3)),
                pltpu.SemaphoreType.DMA((halves, n_rows)),
                pltpu.SemaphoreType.DMA((2, halves, n_rows)),
                pltpu.SemaphoreType.DMA((2, halves, n_rows)),
                pltpu.SemaphoreType.DMA((2, halves, n_ranks - 1)),
                pltpu.SemaphoreType.DMA((2, halves, n_ranks - 1)),
            ],
            compiler_params=pltpu.CompilerParams(collective_id=0, has_side_effects=True, vmem_limit_bytes=60 * 1024 * 1024),
            name="decode",
        )(latent, weights, conv_biases, gn_gammas, gn_betas)

    return jax.shard_map(local_fn, mesh=mesh, in_specs=(frame_spec, P(), P(), P(), P()), out_specs=frame_spec, check_vma=False)
```

```python
import functools

import jax
import jax.numpy as jnp
from jax import lax
from jax.experimental import pallas as pl
from jax.experimental.pallas import tpu as pltpu
from jax.sharding import PartitionSpec as P

GROUPS = 32
NORM_EPS = 1e-6
N_LAYERS = 4
HALF = 256
MESH = pl.DeviceIdType.MESH


def interleave(long, short):
    if not short:
        return list(long)
    out, taken = [], 0
    for idx, job in enumerate(long):
        due = (idx * len(short)) // max(len(long), 1) + 1
        while taken < min(due, len(short)):
            out.append(short[taken])
            taken += 1
        out.append(job)
    return out + list(short[taken:])


def make_kernel(n_ranks, n_frames, n_rows, n_cols, n_chans):
    width = n_chans // GROUPS
    elem_count = float(n_ranks * n_frames * n_rows * n_cols * width)
    halves = n_chans // HALF
    pairs = [((row,), (row + 1,)) for row in range(1, n_rows - 1, 2)] + [((0,), (n_rows - 1,))]
    block = n_frames * n_cols

    def kernel(latent, weights, biases, gammas, betas, out, wbuf, act_0l, act_0c, act_0r, act_1l, act_1c, act_1r, raw, part, stat,
               sums, coef, w_sem, lat_sem, halo_send, halo_recv, st_send, st_recv):
        acts = ({-1: act_0l, 0: act_0c, 1: act_0r}, {-1: act_1l, 0: act_1c, 1: act_1r})
        me = lax.axis_index("cp")
        is_first = me == 0
        nought = lax.rem(me * (me + 1), 2)

        def weight_copy(layer, slot, k):
            return pltpu.make_async_copy(weights.at[layer, pl.ds(9 * k, 9)], wbuf.at[slot, pl.ds(9 * k, 9)], w_sem.at[slot, k])

        def latent_copy(half, row):
            return pltpu.make_async_copy(latent.at[:, row, :, pl.ds(half * HALF, HALF)],
                                         raw.at[0, half, row, pl.ds(2, n_frames)], lat_sem.at[half, row])

        def out_copy(half, row):
            return pltpu.make_async_copy(raw.at[0, half, row, pl.ds(2, n_frames)],
                                         out.at[:, row, :, pl.ds(half * HALF, HALF)], lat_sem.at[half, row])

        def halo_copy(layer, slot, half, row):
            return pltpu.make_async_remote_copy(
                src_ref=raw.at[slot, half, row, pl.ds(2, n_frames)], dst_ref=raw.at[slot, half, row, pl.ds(0, n_frames)],
                send_sem=halo_send.at[slot, half, row], recv_sem=halo_recv.at[slot, half, row],
                device_id={"cp": lax.rem(me + 1, n_ranks)}, device_id_type=MESH)

        def stat_copy(layer, half, hop):
            turn = layer % 2 if isinstance(layer, int) else lax.rem(layer, 2)
            return pltpu.make_async_remote_copy(
                src_ref=stat.at[layer, half, me], dst_ref=stat.at[layer, half, me],
                send_sem=st_send.at[turn, half, hop - 1], recv_sem=st_recv.at[turn, half, hop - 1],
                device_id={"cp": lax.rem(me + hop, n_ranks)}, device_id_type=MESH)

        def send_stats(layer, half):
            stat[layer, half, me, 0:1, :] = jnp.sum(sums[half, 0], axis=0, keepdims=True)
            stat[layer, half, me, 1:2, :] = jnp.sum(sums[half, 1], axis=0, keepdims=True)
            for hop in range(1, n_ranks):
                stat_copy(layer, half, hop).start()

        def clear_sums(half):
            sums[half] = jnp.zeros(sums.shape[1:], sums.dtype)

        def add_sums(val, half):
            slabs = val.reshape(n_cols // 8, 8, val.shape[-1])
            sums[half, 0] += jnp.sum(slabs, axis=0)
            sums[half, 1] += jnp.sum(slabs * slabs, axis=0)

        def take_stats(layer, param, half):
            for hop in range(1, n_ranks):
                stat_copy(layer, half, hop).wait_recv()
            total = stat[layer, half, 0]
            for rank in range(1, n_ranks):
                total = total + stat[layer, half, rank]
            lane = lax.broadcasted_iota(jnp.int32, total.shape, 1)
            step = 1
            while step < width:
                lower = pltpu.roll(total, step, 1)
                upper = pltpu.roll(total, HALF - step, 1)
                total = total + jnp.where(lax.rem(lax.div(lane, step), 2) == 0, upper, lower)
                step *= 2
            cols = pl.ds(half * HALF, HALF)
            mean = total[0:1] * (1.0 / elem_count)
            var = total[1:2] * (1.0 / elem_count) - mean * mean
            scale = lax.rsqrt(var + NORM_EPS) * gammas[pl.ds(param, 1), cols]
            coef[half, 0:1, :] = scale
            coef[half, 1:2, :] = betas[pl.ds(param, 1), cols] - mean * scale

        def act_piece(slot, half, row, frame):
            left, centre, right = acts[half][-1], acts[half][0], acts[half][1]
            src = jnp.where(is_first, 2, frame) if frame < 2 else frame
            val = raw[slot, half, row, src].astype(jnp.float32)
            normed = (val * coef[half, 0:1] + coef[half, 1:2]).astype(jnp.bfloat16).astype(jnp.float32)
            arg = 0.5 * normed
            res = arg * jnp.tanh(arg) + arg
            centre[row, frame] = res.astype(jnp.bfloat16)
            edge = lax.broadcasted_iota(jnp.int32, (16, HALF), 0)
            moved = pltpu.roll(res, 1, 0)
            left[row, frame, 0:16] = jnp.where(edge == 0, 0.0, moved[:16]).astype(jnp.bfloat16)
            left[row, frame, 16:n_cols] = moved[16:].astype(jnp.bfloat16)
            moved = pltpu.roll(res, n_cols - 1, 0)
            right[row, frame, 0:n_cols - 16] = moved[:n_cols - 16].astype(jnp.bfloat16)
            right[row, frame, n_cols - 16:n_cols] = jnp.where(edge == 15, 0.0, moved[n_cols - 16:]).astype(jnp.bfloat16)

        def act_jobs(slot, half, row, local):
            return [functools.partial(act_piece, slot, half, row, frame) for frame in ((2, 3) if local else (0, 1))]

        for half in range(halves):
            for row in range(n_rows):
                latent_copy(half, row).start()
        for k in (2, 1, 0):
            weight_copy(0, 0, k).start()
        barrier = pltpu.get_barrier_semaphore()
        for hop in range(1, n_ranks):
            pl.semaphore_signal(barrier, inc=1, device_id={"cp": lax.rem(me + hop, n_ranks)}, device_id_type=MESH)
        for half in range(halves):
            clear_sums(half)
            for row in range(n_rows):
                latent_copy(half, row).wait()
                for frame in range(n_frames):
                    add_sums(raw[0, half, row, 2 + frame].astype(jnp.float32), half)
        pl.semaphore_wait(barrier, n_ranks - 1)
        for half in range(halves):
            send_stats(0, half)
        for half in range(halves):
            for row in range(n_rows):
                halo_copy(0, 0, half, row).start()
        take_stats(0, 0, 0)
        for row in range(2):
            for job in act_jobs(0, 0, row, True):
                job()

        def layer_step(layer, carry):
            slot = lax.rem(layer, 2)
            other = 1 - slot
            adds_input = slot == 1
            last = layer == N_LAYERS - 1

            @pl.when(jnp.logical_not(last))
            def _():
                for k in (2, 1, 0):
                    weight_copy(layer + 1, other, k).start()

            vals = {}

            def accumulate(key, lhs, tap, in_half, cols, where=None):
                term = jnp.dot(lhs, wbuf[slot if where is None else where, tap, pl.ds(in_half * HALF, HALF), cols], preferred_element_type=jnp.float32)
                vals[key] = term if key not in vals else vals[key] + term

            def taps(k):
                return [(di, dj, 9 * k + 3 * (di + 1) + dj + 1) for dj in (-1, 0, 1) for di in (0, 1, -1)]

            def row_tile(key, row, k, di, dj, tap, in_half):
                lhs = acts[in_half][dj][row + di, pl.ds(k, n_frames)].reshape(block, HALF)
                accumulate(key, lhs, tap, in_half, pl.ds(0, n_chans))

            def row_chain(key, row, k, in_half):
                return [functools.partial(row_tile, key, row, k, di, dj, tap, in_half)
                        for di, dj, tap in taps(k) if 0 <= row + di < n_rows]

            def set_tile(tag, rows, di, dj, tap, in_half, out_half):
                inside = [row for row in rows if 0 <= row + di < n_rows]
                count = len(inside)
                lhs = acts[in_half][dj][pl.ds(inside[0] + di, count), pl.ds(tap // 9, n_frames)].reshape(count * block, HALF)
                accumulate((tag, rows), lhs, tap, in_half, pl.ds(out_half * HALF, HALF))

            def pair_chain(tag, pair, k, in_half, out_half):
                streams = [[functools.partial(set_tile, tag, rows, di, dj, tap, in_half, out_half) for di, dj, tap in taps(k)
                            if any(0 <= row + di < n_rows for row in rows)] for rows in pair]
                return [job for jobs in zip(*streams) for job in jobs]

            def keep_piece(key, row, frame, first, cols):
                span = slice(frame * n_cols, (frame + 1) * n_cols)
                got = vals[key][span]
                part[row, span, cols] = got if first else part[row, span, cols] + got

            def keep_jobs(key, row, first, half=None):
                cols = pl.ds(0, n_chans) if half is None else pl.ds(half * HALF, HALF)
                return [functools.partial(keep_piece, key, row, frame, first, cols) for frame in range(n_frames)]

            def out_piece(tag, rows, row, half, frame):
                span = slice(frame * n_cols, (frame + 1) * n_cols)
                base = (row - rows[0]) * block + frame * n_cols
                cols = pl.ds(half * HALF, HALF)
                got = jnp.where(nought == 0, vals[tag, rows][base:base + n_cols], 0.0) + part[row, span, cols] + biases[pl.ds(layer, 1), cols]
                inner = got.astype(jnp.bfloat16).astype(jnp.float32)
                held = raw[other, half, row, 2 + frame].astype(jnp.float32)
                new = jnp.where(adds_input, held + inner, inner).astype(jnp.bfloat16)
                raw[other, half, row, 2 + frame] = new
                add_sums(new.astype(jnp.float32), half)

            def out_jobs(tag, pair, half):
                return [functools.partial(out_piece, tag, rows, row, half, frame)
                        for rows in pair for row in rows for frame in range(n_frames)]

            def send_jobs(half, rows):
                return [lambda row=row: halo_copy(layer + 1, other, half, row).start() for row in rows]

            def halo_jobs(half, row):
                return [lambda: halo_copy(layer, slot, half, row).wait_recv()] + act_jobs(slot, half, row, False)

            def run(tiles, side=()):
                for job in interleave(tiles, list(side)):
                    job()

            def sent(row):
                halo_copy(layer, slot, 0, row).wait_send()

            later = []
            spread = [[(0, 1)], [(2,)], [(3,)], [(4,)], [(5,)]]
            for k in (2, 1, 0):
                weight_copy(layer, slot, k).wait()
                for row in range(n_rows):
                    key = ("row", k, row)
                    side = later
                    if k == 2 and row + 2 < n_rows:
                        side = side + act_jobs(slot, 0, row + 2, True)
                    if k == 2 and row >= n_rows - 2:
                        side = side + halo_jobs(0, row - n_rows + 2)
                    if k == 1 and row + 2 < n_rows:
                        side = side + halo_jobs(0, row + 2)
                    if k == 0 and row == 1:
                        side = side + [functools.partial(take_stats, layer, layer, 1)]
                    if k == 0 and row >= 1:
                        for got in (rows for group in spread[row - 1] for rows in group):
                            side = side + act_jobs(slot, 1, got, True) + [functools.partial(sent, got)]
                    run(row_chain(key, row, k, 0), side)
                    later = keep_jobs(key, row, k == 2)

            clear_sums(0)
            for idx, pair in enumerate(pairs):
                tag = ("first", idx)
                ready = [(0, 1, 2, 3), (4, 5), ()][idx]
                run(pair_chain(tag, pair, 2, 1, 0), [job for row in ready for job in halo_jobs(1, row)])
                run(pair_chain(tag, pair, 1, 1, 0), later)
                run(pair_chain(tag, pair, 0, 1, 0))
                later = out_jobs(tag, pair, 0) + (send_jobs(0, (1, 2)) if idx == 0 else [])

            ahead = [functools.partial(take_stats, layer + 1, jnp.minimum(layer + 1, N_LAYERS - 1), 0)]
            ahead = ahead + [job for row in range(2) for job in act_jobs(other, 0, row, True)]

            later = later + [functools.partial(send_stats, layer + 1, 0), functools.partial(clear_sums, 1)]
            later = later + send_jobs(0, (0, 3, 4, 5))
            for idx, pair in enumerate(pairs):
                tag = ("second", idx)
                early = later if idx == 0 else []
                run(pair_chain(tag, pair, 2, 1, 1), early)
                tiles = pair_chain(tag, pair, 1, 1, 1) + pair_chain(tag, pair, 0, 1, 1)
                cut = len(tiles) * 3 // 4 if idx == len(pairs) - 1 else len(tiles)
                run(tiles[:cut], [] if idx == 0 else later)
                run(tiles[cut:], ahead if cut < len(tiles) else [])
                later = out_jobs(tag, pair, 1)
            for job in later:
                job()

            @pl.when(jnp.logical_not(last))
            def _():
                send_stats(layer + 1, 1)

            @pl.when(jnp.logical_not(last))
            def _():
                for row in range(n_rows):
                    halo_copy(layer + 1, other, 1, row).start()

            @pl.when(last)
            def _():
                for half in range(halves):
                    for row in range(n_rows):
                        out_copy(half, row).start()

            for half in range(halves):
                for row in range(n_rows if half else 0):
                    halo_copy(layer, slot, half, row).wait_send()
                for hop in range(1, n_ranks):
                    stat_copy(layer, half, hop).wait_send()
            return carry

        lax.fori_loop(0, N_LAYERS, layer_step, 0)
        for hop in range(1, n_ranks):
            stat_copy(N_LAYERS, 0, hop).wait_send()
        for row in range(n_rows):
            halo_copy(N_LAYERS, 0, 0, row).wait_send()
            halo_copy(N_LAYERS, 0, 0, row).wait_recv()
        for half in range(halves):
            for row in range(n_rows):
                out_copy(half, row).wait()

    return kernel


def solution(mesh):
    n_ranks = mesh.shape["cp"]
    frame_spec = P(("dp", "cp"))

    def local_fn(latent, conv_kernels, conv_biases, gn_gammas, gn_betas):
        n_frames, n_rows, n_cols, n_chans = latent.shape
        weights = conv_kernels.reshape(N_LAYERS, 27, n_chans, n_chans)
        halves = n_chans // HALF
        act_shape = pltpu.VMEM((n_rows, 4, n_cols, HALF), jnp.bfloat16)
        return pl.pallas_call(
            make_kernel(n_ranks, n_frames, n_rows, n_cols, n_chans),
            out_shape=jax.ShapeDtypeStruct(latent.shape, latent.dtype),
            in_specs=[pl.BlockSpec(memory_space=pl.ANY)] * 2 + [pl.BlockSpec(memory_space=pltpu.VMEM)] * 3,
            out_specs=pl.BlockSpec(memory_space=pl.ANY),
            scratch_shapes=[
                pltpu.VMEM((2, 27, n_chans, n_chans), jnp.bfloat16),
                act_shape, act_shape, act_shape, act_shape, act_shape, act_shape,
                pltpu.VMEM((2, halves, n_rows, 4, n_cols, HALF), jnp.bfloat16),
                pltpu.VMEM((n_rows, n_frames * n_cols, n_chans), jnp.float32),
                pltpu.VMEM((N_LAYERS + 1, halves, n_ranks, 2, HALF), jnp.float32),
                pltpu.VMEM((halves, 2, 8, HALF), jnp.float32),
                pltpu.VMEM((halves, 2, HALF), jnp.float32),
                pltpu.SemaphoreType.DMA((2, 3)),
                pltpu.SemaphoreType.DMA((halves, n_rows)),
                pltpu.SemaphoreType.DMA((2, halves, n_rows)),
                pltpu.SemaphoreType.DMA((2, halves, n_rows)),
                pltpu.SemaphoreType.DMA((2, halves, n_ranks - 1)),
                pltpu.SemaphoreType.DMA((2, halves, n_ranks - 1)),
            ],
            compiler_params=pltpu.CompilerParams(collective_id=0, has_side_effects=True, vmem_limit_bytes=60 * 1024 * 1024),
            name="decode",
        )(latent, weights, conv_biases, gn_gammas, gn_betas)

    return jax.shard_map(local_fn, mesh=mesh, in_specs=(frame_spec, P(), P(), P(), P()), out_specs=frame_spec, check_vma=False)
```
